32 devices in a mesh: shot: 8 (over z, y), grp: 4 (over x, core).
Axes of the slice: x: 2, y: 2, z: 4, core: 2. Of those that a mesh axis runs over, the one named last changes fastest.
Arguments:
- offsets: bfloat16 [6144, 32, 512], P(('shot', 'grp')), may hold values from -500 to 500
- slant_weights: bfloat16 [64, 32], replicated, may hold values from -1 to 1
- live: int32 [6144, 64], P(('shot', 'grp')), may hold values from 0 to 1, as said below
- block_tile: int32 [3072, 1], P(('shot', 'grp')), may hold values from 0 to 7; in each aligned block of 96 rows (0 to 95, 96 to 191, ...) at most 13 rows name the same one
- image_slot: int32 [3072], P(('shot', 'grp')), may hold values from 0 to 15
Outputs:
- image: bfloat16 [128, 128, 512], P(('shot', 'grp'))
The draws below stay inside these ranges and needn't reach their ends.
Inputs may be any that keep to these rules, and one draw needn't show every extreme that they name: Each position's live angles are 0 up to a cutoff minus 1, the cutoff at least 16; the first position of every 192 positions keeps all 64 angles. `block_tile`: among the 96 blocks of one device no tile is named more than 13 times.
All inputs are finite; a program needn't handle non-finite values.
Results may differ from the reference program's by a relative error of at most 0.0049.
Values may be sent and summed in bfloat16 or wider, within the bound.
A program may use at most 192 MiB of HBM per device.

```python
import math
import jax
import jax.numpy as jnp
import numpy as np
from jax import lax

ANG = 64
H = 32
Z = 512
TRB = 128
BLK_DEV = 96
IMG_DEV = 4
CAP = 13
POS_DEV = 192
POSITIONS = 6144
BLOCKS = 3072
IT = 16
IMAGE_BLOCKS = 128
N_SHOT = 8
N_GRP = 4
DEVICES = 32


def draw_offsets(key, part):
    keys = jax.random.split(jax.random.fold_in(key, 11), 3)
    row_scale = jnp.exp(jax.random.uniform(keys[1], (POSITIONS, 1, 1), jnp.float32) * jnp.log(10.0))
    depth_scale = jnp.exp(jax.random.uniform(keys[2], (1, 1, Z), jnp.float32) * jnp.log(10.0))
    place = jnp.arange(POSITIONS, dtype=jnp.float32) / max(POSITIONS - 1, 1)
    base = jnp.clip(jax.random.normal(keys[0], (POSITIONS, H, Z), jnp.float32), -6.0, 6.0)
    ramp = 1.0 + 2.0 * place
    values = 0.1 * base * row_scale * depth_scale * ramp[:, None, None]
    return values.astype(jnp.bfloat16)


def draw_live(key, part):
    cutoff = jax.random.randint(jax.random.fold_in(key, 23), (POSITIONS,), ANG // 4, ANG + 1)
    first = jnp.arange(POSITIONS) % POS_DEV == 0
    cutoff = jnp.where(first, ANG, cutoff)
    return (jnp.arange(ANG)[None, :] < cutoff[:, None]).astype(jnp.int32)


def place_ends(drawn, key, low, top_value):
    spot = [jax.random.randint(jax.random.fold_in(key, axis), (), 0, length) for axis, length in enumerate(drawn.shape)]
    longest = drawn.shape.index(max(drawn.shape))
    next_to = spot[:longest] + [(spot[longest] + 1) % drawn.shape[longest]] + spot[longest + 1:]
    return drawn.at[tuple(spot)].set(low).at[tuple(next_to)].set(top_value)


def deal_out(key, own, number, rows, number_of, top, most, lean):
    order = jax.random.permutation(key, number_of)
    crowded, usual = shares(number_of, rows * top, most, lean, True), shares(number_of, rows * top, most, lean, False)
    places = jnp.arange(number_of)

    def named(lengths, rotation):
        used = int((lengths > 0).sum())
        fixed = max(1, used // 4)
        moved = fixed + (places - fixed + rotation * (used - fixed)) % max(1, number_of - fixed)
        return jnp.zeros((number_of,), jnp.int32).at[order[jnp.where(places < fixed, places, moved)]].set(jnp.asarray(lengths, jnp.int32))

    lengths = jnp.where(number % 4 == 0, named(crowded, number // 4), named(usual, number - number // 4 - 1))
    mixed = jax.random.permutation(jax.random.fold_in(own, 3), number_of)
    giver, receiver = mixed[0:number_of // 2 * 2:2], mixed[1:number_of // 2 * 2:2]
    margin = jnp.minimum(lengths[giver] - 1, most - lengths[receiver]) // 2
    margin = jnp.where((giver == order[0]) | (receiver == order[0]) | (lengths[receiver] == 0), 0, jnp.maximum(margin, 0))
    moved = jax.random.randint(jax.random.fold_in(own, 4), (number_of // 2,), 0, 1 << 20) % (margin + 1)
    lengths = lengths.at[giver].add(-moved).at[receiver].add(moved)
    labels = jnp.searchsorted(jnp.cumsum(lengths), jnp.arange(rows * top), side="right").astype(jnp.int32)
    table = labels.reshape(top, rows).T
    table = table[jax.random.permutation(jax.random.fold_in(own, 1), rows)]
    rotation = jax.random.randint(jax.random.fold_in(own, 2), (rows, 1), 0, top)
    return jnp.take_along_axis(table, (jnp.arange(top)[None, :] + rotation) % top, axis=1)


def shares(number_of, total, reach, lean, full):
    weights = [(1 << 20) // math.isqrt(standing ** lean) + 1 for standing in range(1, number_of + 1)]
    largest = reach if full else min(reach, max(-(-total // number_of), total * weights[0] // sum(weights)))
    least = 1 if total - largest >= number_of - 1 else 0
    counts, spare = [largest] + [least] * (number_of - 1), total - largest - least * (number_of - 1)
    while spare > 0:
        movable = [i for i in range(1, number_of) if counts[i] < largest] or [i for i in range(1, number_of) if counts[i] < reach]
        mass, budget = sum([weights[i] for i in movable]), spare
        for i in movable:
            more = min(reach - counts[i], max(1, budget * weights[i] // mass), spare)
            counts[i] = counts[i] + more
            spare = spare - more
    return np.array(counts)


def noise(rng, shape, width, most, kind=jnp.bfloat16):
    return jnp.clip(width * jax.random.normal(rng, shape, jnp.float32), -most, most).astype(kind)


def setup_inputs(seed: int = 0) -> dict:
    key_list = jax.random.split(jax.random.key(seed), 6)
    offsets = draw_offsets(jax.random.fold_in(key_list[5], 71), 0)
    slant_weights = noise(key_list[1], (ANG, H), H ** -0.5, 1.0)
    live = draw_live(jax.random.fold_in(key_list[5], 71), 0)
    block_tile_keys = jax.random.split(jax.random.fold_in(key_list[3], 1), BLOCKS // BLK_DEV)
    block_tile_turns = jax.random.permutation(jax.random.fold_in(key_list[3], 3), BLOCKS // BLK_DEV)
    block_tile = jax.vmap(lambda own, number: deal_out(jax.random.fold_in(key_list[3], 2), own, number, BLK_DEV, N_SHOT, 1, CAP, 1))(block_tile_keys, block_tile_turns).reshape((BLOCKS, 1))
    image_slot = place_ends(jax.random.randint(key_list[4], (BLOCKS,), 0, IT), jax.random.fold_in(key_list[4], 1), 0, IT - 1).astype(jnp.int32)
    return {"offsets": offsets, "slant_weights": slant_weights, "live": live, "block_tile": block_tile, "image_slot": image_slot}


def reference(offsets, slant_weights, live, block_tile, image_slot):
    tile_rows = IMG_DEV * N_GRP
    weights = slant_weights.astype(jnp.float32)
    shards = (offsets.reshape(DEVICES, POS_DEV, H, Z), live.reshape(DEVICES, POS_DEV, ANG), block_tile.reshape(DEVICES, BLK_DEV), image_slot.reshape(DEVICES, BLK_DEV))

    def advance(state_in, pieces):
        stacked, square_sum, live_count = state_in
        shard_off, shard_live, shard_tile, shard_slot = pieces
        live_mask = shard_live.astype(jnp.float32)
        slanted = jnp.einsum('ah,phz->paz', weights, shard_off.astype(jnp.float32))
        angles = (slanted * live_mask[:, :, None]).astype(jnp.bfloat16)
        widened = angles.astype(jnp.float32)
        square_sum = square_sum + lax.optimization_barrier(jnp.sum(widened * widened, axis=(0, 2)))
        live_count = live_count + lax.optimization_barrier(jnp.sum(live_mask, axis=0))
        targets = (shard_tile.astype(jnp.int32) * tile_rows + shard_slot.astype(jnp.int32)).astype(jnp.int32)
        stacked = stacked.at[targets].add(widened.reshape(BLK_DEV, TRB, Z))
        return ((stacked, square_sum, live_count), None)
    initial = (jnp.zeros((IMAGE_BLOCKS, TRB, Z), jnp.float32), jnp.zeros((ANG,), jnp.float32), jnp.zeros((ANG,), jnp.float32))
    (stacked, square_sum, live_count), unused = lax.scan(advance, initial, shards)
    angle_gain = lax.rsqrt(square_sum / (Z * live_count) + 1e-06)
    trace_gain = jnp.tile(angle_gain, 2)
    return (stacked * trace_gain[None, :, None]).astype(jnp.bfloat16)
```

```python
import functools

import jax
import jax.numpy as jnp
from jax import lax
from jax.experimental import pallas as pl
from jax.experimental.pallas import tpu as pltpu
from jax.sharding import PartitionSpec as P

IMG_DEV = 4
PAIR = 2
LANES = 128
UNROLL = 8
MESH = pl.DeviceIdType.MESH


def place(grp):
    shot, g = lax.axis_index("shot"), lax.axis_index("grp")
    return lax.div(shot, PAIR), lax.rem(shot, PAIR) * grp + g


def at(plane, spot, grp):
    return (plane * PAIR + lax.div(spot, grp), lax.rem(spot, grp))


def share(spot, width, depth):
    start = spot * width
    return lax.div(start, depth), pl.multiple_of(lax.rem(start, depth), LANES)


def exchange_kernel(grp, off, aux, raw_in, aux_in, stage, send, recv, asend, arecv, lsem):
    size = PAIR * grp
    plane, spot = place(grp)
    depth, width = off.shape[3], raw_in.shape[3]
    barrier = pltpu.get_barrier_semaphore()
    for r in range(1, size):
        pl.semaphore_signal(
            barrier, inc=1, device_id=at(plane, lax.rem(spot + r, size), grp), device_id_type=MESH
        )
    pl.semaphore_wait(barrier, size - 1)
    copies = []
    for r in range(1, size):
        peer = lax.rem(spot + r, size)
        j, first = share(peer, width, depth)
        dev = at(plane, peer, grp)
        copies.append(
            pltpu.make_async_remote_copy(
                src_ref=aux,
                dst_ref=aux_in.at[spot],
                send_sem=asend.at[r - 1],
                recv_sem=arecv.at[r - 1],
                device_id=dev,
                device_id_type=MESH,
            )
        )
        copies.append(
            pltpu.make_async_remote_copy(
                src_ref=off.at[:, j, :, pl.ds(first, width)],
                dst_ref=raw_in.at[spot],
                send_sem=send.at[r - 1],
                recv_sem=recv.at[r - 1],
                device_id=dev,
                device_id_type=MESH,
            )
        )
    for copy in copies:
        copy.start()
    j, first = share(spot, width, depth)
    a = pltpu.make_async_copy(off.at[:, j, :, pl.ds(first, width)], stage, lsem.at[0])
    c = pltpu.make_async_copy(aux, aux_in.at[spot], lsem.at[1])
    a.start()
    c.start()
    a.wait()
    b = pltpu.make_async_copy(stage, raw_in.at[spot], lsem.at[2])
    b.start()
    b.wait()
    c.wait()
    for copy in copies:
        copy.wait()


def stack_kernel(steps, half, aux, w, raw, part, mom, acc, sums):
    c, s = pl.program_id(0), pl.program_id(1)
    angles = w.shape[0]

    @pl.when(s == 0)
    def _():
        acc[...] = jnp.zeros_like(acc)

    @pl.when((s == 0) & (c == 0))
    def _():
        sums[...] = jnp.zeros_like(sums)

    @pl.when(s < steps)
    def _():
        row = lax.broadcasted_iota(jnp.int32, (angles, LANES), 0)
        weights = w[...]
        mine = 1 + half[0]

        def body(i, carry):
            square, count = carry
            first = i * UNROLL
            x = jnp.concatenate([raw[0, first + t] for t in range(UNROLL)], axis=1)
            y = jnp.dot(weights, x, preferred_element_type=jnp.float32)
            for t in range(UNROLL):
                alive = row < aux[s, mine, first + t]
                slanted = jnp.where(alive, y[:, t * LANES : (t + 1) * LANES], 0.0)
                slanted = slanted.astype(jnp.bfloat16).astype(jnp.float32)
                square += slanted * slanted
                count += jnp.where(alive, 1.0, 0.0)
                k = aux[s, 0, first + t]
                acc[k] += slanted
            return square, count

        square, count = lax.fori_loop(0, raw.shape[1] // UNROLL, body, (sums[0], sums[1]))
        sums[0] = square
        sums[1] = count

    @pl.when(s >= steps)
    def _():
        rows = part.shape[0]
        part[...] = acc[pl.ds((s - steps) * rows, rows)].astype(jnp.bfloat16)
        lane = lax.broadcasted_iota(jnp.int32, (angles, LANES), 1)
        square = jnp.sum(sums[0], axis=1, keepdims=True)
        count = jnp.sum(sums[1], axis=1, keepdims=True)
        mom[...] = jnp.where(lane == 0, square, jnp.where(lane == 1, count, 0.0))


def gather_kernel(
    grp, part, mom, out, zin, own, fin, pin, qin, half_sum, zs, zr, ps, pr, qs, qr, fs, fr, lsem
):
    size = PAIR * grp
    planes = zin.shape[0] + 1
    plane, spot = place(grp)
    rows, width, depth = own.shape[0], own.shape[2], out.shape[2]
    angles = own.shape[1]
    barrier = pltpu.get_barrier_semaphore()
    for r in range(1, size):
        pl.semaphore_signal(
            barrier, inc=1, device_id=at(plane, lax.rem(spot + r, size), grp), device_id_type=MESH
        )
    for r in range(1, planes):
        pl.semaphore_signal(
            barrier, inc=1, device_id=at(lax.rem(plane + r, planes), spot, grp), device_id_type=MESH
        )
    pl.semaphore_wait(barrier, size + planes - 2)

    near = [
        pltpu.make_async_remote_copy(
            src_ref=mom,
            dst_ref=pin.at[r - 1],
            send_sem=ps.at[r - 1],
            recv_sem=pr.at[r - 1],
            device_id=at(plane, lax.rem(spot + r, size), grp),
            device_id_type=MESH,
        )
        for r in range(1, size)
    ]
    for copy in near:
        copy.start()
    mine = pltpu.make_async_copy(part.at[pl.ds(plane * rows, rows)], own, lsem.at[0])
    mine.start()
    far = []
    for r in range(1, planes):
        target = lax.rem(plane + r, planes)
        far.append(
            pltpu.make_async_remote_copy(
                src_ref=part.at[pl.ds(target * rows, rows)],
                dst_ref=zin.at[r - 1],
                send_sem=zs.at[r - 1],
                recv_sem=zr.at[r - 1],
                device_id=at(target, spot, grp),
                device_id_type=MESH,
            )
        )
    total = mom[...]
    for copy in near:
        copy.wait()
    for r in range(1, size):
        total += pin[r - 1]
    half_sum[...] = total
    wide = [
        pltpu.make_async_remote_copy(
            src_ref=half_sum,
            dst_ref=qin.at[r - 1],
            send_sem=qs.at[r - 1],
            recv_sem=qr.at[r - 1],
            device_id=at(lax.rem(plane + r, planes), spot, grp),
            device_id_type=MESH,
        )
        for r in range(1, planes)
    ]
    for copy in wide:
        copy.start()
    for copy in far:
        copy.start()
    for copy in wide:
        copy.wait()
    total = half_sum[...]
    for r in range(1, planes):
        total += qin[r - 1]
    gain = lax.rsqrt(total[:, 0:1] / total[:, 1:2] + 1e-06)
    gain = jnp.broadcast_to(gain, (angles, width))
    mine.wait()
    for copy in far:
        copy.wait()

    def body(i, _):
        value = own[i].astype(jnp.float32)
        for r in range(1, planes):
            value += zin[r - 1, i].astype(jnp.float32)
        fin[i] = (value * gain).astype(jnp.bfloat16)
        return 0

    lax.fori_loop(0, rows, body, 0)

    each = rows // size
    j, first = share(spot, width, depth)
    view = out.at[:, pl.ds(pl.multiple_of(j * angles, angles), angles), pl.ds(first, width)]
    last = pltpu.make_async_copy(fin.at[pl.ds(spot * each, each)], view, lsem.at[1])
    final = []
    for r in range(1, size):
        peer = lax.rem(spot + r, size)
        final.append(
            pltpu.make_async_remote_copy(
                src_ref=fin.at[pl.ds(peer * each, each)],
                dst_ref=view,
                send_sem=fs.at[r - 1],
                recv_sem=fr.at[r - 1],
                device_id=at(plane, peer, grp),
                device_id_type=MESH,
            )
        )
    for copy in final:
        copy.start()
    last.start()
    last.wait()
    for copy in final:
        copy.wait()


def local(offsets, slant_weights, live, block_tile, image_slot):
    shots, grp = lax.axis_size("shot"), lax.axis_size("grp")
    planes, size = shots // PAIR, PAIR * grp
    blocks = block_tile.shape[0]
    hs, depth = offsets.shape[1:]
    angles = slant_weights.shape[0]
    width = 2 * depth // size
    tile_rows = IMG_DEV * grp
    images = shots * tile_rows
    per_plane = images // planes
    any_space = pl.BlockSpec(memory_space=pl.ANY)
    vmem = pl.BlockSpec(memory_space=pltpu.VMEM)
    smem = pl.BlockSpec(memory_space=pltpu.SMEM)
    dma = pltpu.SemaphoreType.DMA

    cutoff = jnp.sum(live.reshape(blocks, 2, angles), axis=2)
    image = block_tile[:, 0] * tile_rows + image_slot
    aux = jnp.concatenate([image[None], cutoff.T], axis=0)
    aux = jnp.pad(aux, ((0, 5), (0, -blocks % LANES)))

    raw_in, aux_in = pl.pallas_call(
        functools.partial(exchange_kernel, grp),
        out_shape=(
            jax.ShapeDtypeStruct((size, blocks, hs, width), jnp.bfloat16),
            jax.ShapeDtypeStruct((size,) + aux.shape, jnp.int32),
        ),
        in_specs=[any_space, vmem],
        out_specs=(any_space, vmem),
        scratch_shapes=[
            pltpu.VMEM((blocks, hs, width), jnp.bfloat16),
            dma((size - 1,)),
            dma((size - 1,)),
            dma((size - 1,)),
            dma((size - 1,)),
            dma((3,)),
        ],
        compiler_params=pltpu.CompilerParams(collective_id=0, has_side_effects=True),
        name="exchange",
    )(offsets.reshape(blocks, 2, hs, depth), aux)

    spot = lax.rem(lax.axis_index("shot"), PAIR) * grp + lax.axis_index("grp")
    half = (spot * width // depth).astype(jnp.int32).reshape(1)
    part, mom = pl.pallas_call(
        functools.partial(stack_kernel, size),
        grid=(width // LANES, size + planes),
        out_shape=(
            jax.ShapeDtypeStruct((images, angles, width), jnp.bfloat16),
            jax.ShapeDtypeStruct((angles, LANES), jnp.float32),
        ),
        in_specs=[
            smem,
            smem,
            pl.BlockSpec((angles, hs), lambda c, s: (0, 0)),
            pl.BlockSpec(
                (1, blocks, hs, LANES), lambda c, s: (jnp.minimum(s, size - 1), 0, 0, c)
            ),
        ],
        out_specs=(
            pl.BlockSpec(
                (per_plane, angles, LANES), lambda c, s: (jnp.maximum(s - size, 0), 0, c)
            ),
            pl.BlockSpec((angles, LANES), lambda c, s: (0, 0)),
        ),
        scratch_shapes=[
            pltpu.VMEM((images, angles, LANES), jnp.float32),
            pltpu.VMEM((2, angles, LANES), jnp.float32),
        ],
        compiler_params=pltpu.CompilerParams(vmem_limit_bytes=60 * 1024 * 1024),
        name="stack",
    )(half, aux_in, slant_weights, raw_in)

    moments = (angles, LANES)
    return pl.pallas_call(
        functools.partial(gather_kernel, grp),
        out_shape=jax.ShapeDtypeStruct((IMG_DEV, 2 * angles, depth), jnp.bfloat16),
        in_specs=[any_space, vmem],
        out_specs=any_space,
        scratch_shapes=[
            pltpu.VMEM((planes - 1, per_plane, angles, width), jnp.bfloat16),
            pltpu.VMEM((per_plane, angles, width), jnp.bfloat16),
            pltpu.VMEM((per_plane, angles, width), jnp.bfloat16),
            pltpu.VMEM((size - 1,) + moments, jnp.float32),
            pltpu.VMEM((planes - 1,) + moments, jnp.float32),
            pltpu.VMEM(moments, jnp.float32),
            dma((planes - 1,)),
            dma((planes - 1,)),
            dma((size - 1,)),
            dma((size - 1,)),
            dma((planes - 1,)),
            dma((planes - 1,)),
            dma((size - 1,)),
            dma((size - 1,)),
            dma((2,)),
        ],
        compiler_params=pltpu.CompilerParams(
            collective_id=1, has_side_effects=True, vmem_limit_bytes=60 * 1024 * 1024
        ),
        name="gather",
    )(part, mom)


def solution(mesh):
    placed = (
        P(("shot", "grp"), None, None),
        P(),
        P(("shot", "grp"), None),
        P(("shot", "grp"), None),
        P(("shot", "grp")),
    )
    return jax.shard_map(
        local, mesh=mesh, in_specs=placed, out_specs=P(("shot", "grp"), None, None), check_vma=False
    )
```

```python
import functools

import jax
import jax.numpy as jnp
from jax import lax
from jax.experimental import pallas as pl
from jax.experimental.pallas import tpu as pltpu
from jax.sharding import PartitionSpec as P

IMG_DEV = 4
PAIR = 2
LANES = 128
UNROLL = 8
MESH = pl.DeviceIdType.MESH


def place(grp):
    shot, g = lax.axis_index("shot"), lax.axis_index("grp")
    return lax.div(shot, PAIR), lax.rem(shot, PAIR) * grp + g


def at(plane, spot, grp):
    return (plane * PAIR + lax.div(spot, grp), lax.rem(spot, grp))


def share(spot, width, depth):
    start = spot * width
    return lax.div(start, depth), pl.multiple_of(lax.rem(start, depth), LANES)


def relative(spot, grp, r):
    mid = grp // 2
    pair, rest = lax.div(spot, grp), lax.rem(spot, grp)
    m, c = lax.div(rest, 2), lax.rem(rest, 2)
    rp, rm, rc = r // grp, (r % grp) // 2, r % 2
    pair, m, c = lax.rem(pair + rp, PAIR), lax.rem(m + rm, mid), lax.rem(c + rc, 2)
    return (pair * mid + m) * 2 + c


def orders(grp):
    size = PAIR * grp
    far = list(range(grp + 2, size))
    side = list(range(grp, grp + 2))
    ahead = list(range(2, grp))
    turn = []
    for i in range(max(len(far), len(ahead))):
        for group in (far, side, ahead):
            turn += group[i : i + 1]
    return [1] + turn


def exchange_kernel(
    grp, off, aux, w, part, mom, raw, aux_in, codes, acc, seg, send, recv, asend, arecv, lsem
):
    size = PAIR * grp
    plane, spot = place(grp)
    blocks, depth, width = off.shape[0], off.shape[3], raw.shape[3]
    angles, images = w.shape[0], acc.shape[0]
    j, first = share(spot, width, depth)
    mine = pltpu.make_async_copy(off.at[:, j, :, pl.ds(first, width)], raw.at[0], lsem.at[0])
    mine.start()
    own_codes = pltpu.make_async_copy(aux, codes.at[0], lsem.at[1])
    own_codes.start()
    barrier = pltpu.get_barrier_semaphore()
    for r in range(1, size):
        pl.semaphore_signal(
            barrier, inc=1, device_id=at(plane, relative(spot, grp, r), grp), device_id_type=MESH
        )
    pl.semaphore_wait(barrier, size - 1)
    data, notes = {}, {}
    for r in orders(grp):
        peer = relative(spot, grp, r)
        pj, pfirst = share(peer, width, depth)
        dev = at(plane, peer, grp)
        notes[r] = pltpu.make_async_remote_copy(
            src_ref=aux,
            dst_ref=aux_in.at[r],
            send_sem=asend.at[r - 1],
            recv_sem=arecv.at[r - 1],
            device_id=dev,
            device_id_type=MESH,
        )
        data[r] = pltpu.make_async_remote_copy(
            src_ref=off.at[:, pj, :, pl.ds(pfirst, width)],
            dst_ref=raw.at[r],
            send_sem=send.at[r - 1],
            recv_sem=recv.at[r - 1],
            device_id=dev,
            device_id_type=MESH,
        )
    for r in orders(grp):
        notes[r].start()
    for r in orders(grp):
        data[r].start()

    acc[...] = jnp.zeros_like(acc)
    seg[blocks] = jnp.zeros((angles, width), jnp.float32)
    row = lax.broadcasted_iota(jnp.int32, (angles, width), 0)
    weights = w[...]
    square = jnp.zeros((angles, width), jnp.float32)
    count = jnp.zeros((angles, width), jnp.float32)
    for r in [0] + orders(grp):
        if r:
            notes[r].wait()
            code = pltpu.make_async_copy(aux_in.at[r], codes.at[r], lsem.at[r + 1])
            code.start()
            code.wait()
            data[r].wait()
        else:
            own_codes.wait()
            mine.wait()

        def slant(i, carry, r=r):
            square, count = carry
            start = i * UNROLL
            x = jnp.concatenate([raw[r, start + t] for t in range(UNROLL)], axis=1)
            y = jnp.dot(weights, x, preferred_element_type=jnp.float32)
            for t in range(UNROLL):
                alive = row < codes[r, 1 + j, start + t]
                slanted = jnp.where(alive, y[:, t * width : (t + 1) * width], 0.0)
                slanted = slanted.astype(jnp.bfloat16).astype(jnp.float32)
                square += slanted * slanted
                count += jnp.where(alive, 1.0, 0.0)
                seg[start + t] = slanted + seg[codes[r, 0, start + t]]
            return square, count

        square, count = lax.fori_loop(0, blocks // UNROLL, slant, (square, count))

        def stack(i, _, r=r):
            start = i * UNROLL
            line, column = lax.div(start, LANES), lax.rem(start, LANES)
            for t in range(UNROLL):
                acc[start + t] += seg[codes[r, 3 + line, column + t]]
            return 0

        lax.fori_loop(0, images // UNROLL, stack, 0)

    def narrow(i, _):
        start = pl.multiple_of(i * UNROLL, UNROLL)
        part[pl.ds(start, UNROLL)] = acc[pl.ds(start, UNROLL)].astype(jnp.bfloat16)
        return 0

    lax.fori_loop(0, images // UNROLL, narrow, 0)
    lane = lax.broadcasted_iota(jnp.int32, (angles, LANES), 1)
    square = jnp.sum(square, axis=1, keepdims=True)
    count = jnp.sum(count, axis=1, keepdims=True)
    mom[...] = jnp.where(lane == 0, square, jnp.where(lane == 1, count, 0.0))


def gather_kernel(
    grp, part, mom, out, zin, own, fin, pin, qin, half_sum, zs, zr, ps, pr, qs, qr, fs, fr, lsem
):
    size = PAIR * grp
    planes = zin.shape[0] + 1
    plane, spot = place(grp)
    rows, width, depth = own.shape[0], own.shape[2], out.shape[2]
    angles = own.shape[1]
    barrier = pltpu.get_barrier_semaphore()
    for r in range(1, size):
        pl.semaphore_signal(
            barrier, inc=1, device_id=at(plane, lax.rem(spot + r, size), grp), device_id_type=MESH
        )
    for r in range(1, planes):
        pl.semaphore_signal(
            barrier, inc=1, device_id=at(lax.rem(plane + r, planes), spot, grp), device_id_type=MESH
        )
    pl.semaphore_wait(barrier, size + planes - 2)

    near = [
        pltpu.make_async_remote_copy(
            src_ref=mom,
            dst_ref=pin.at[r - 1],
            send_sem=ps.at[r - 1],
            recv_sem=pr.at[r - 1],
            device_id=at(plane, lax.rem(spot + r, size), grp),
            device_id_type=MESH,
        )
        for r in range(1, size)
    ]
    for copy in near:
        copy.start()
    mine = pltpu.make_async_copy(part.at[pl.ds(plane * rows, rows)], own, lsem.at[0])
    mine.start()
    far = []
    for r in range(1, planes):
        target = lax.rem(plane + r, planes)
        far.append(
            pltpu.make_async_remote_copy(
                src_ref=part.at[pl.ds(target * rows, rows)],
                dst_ref=zin.at[r - 1],
                send_sem=zs.at[r - 1],
                recv_sem=zr.at[r - 1],
                device_id=at(target, spot, grp),
                device_id_type=MESH,
            )
        )
    for copy in far:
        copy.start()
    total = mom[...]
    for copy in near:
        copy.wait()
    for r in range(1, size):
        total += pin[r - 1]
    half_sum[...] = total
    wide = [
        pltpu.make_async_remote_copy(
            src_ref=half_sum,
            dst_ref=qin.at[r - 1],
            send_sem=qs.at[r - 1],
            recv_sem=qr.at[r - 1],
            device_id=at(lax.rem(plane + r, planes), spot, grp),
            device_id_type=MESH,
        )
        for r in range(1, planes)
    ]
    for copy in wide:
        copy.start()
    for copy in wide:
        copy.wait()
    total = half_sum[...]
    for r in range(1, planes):
        total += qin[r - 1]
    gain = lax.rsqrt(total[:, 0:1] / total[:, 1:2] + 1e-06)
    gain = jnp.broadcast_to(gain, (angles, width))
    mine.wait()
    for copy in far:
        copy.wait()

    def body(i, _):
        value = own[i].astype(jnp.float32)
        for r in range(1, planes):
            value += zin[r - 1, i].astype(jnp.float32)
        fin[i] = (value * gain).astype(jnp.bfloat16)
        return 0

    lax.fori_loop(0, rows, body, 0)

    each = rows // size
    j, first = share(spot, width, depth)
    view = out.at[:, pl.ds(pl.multiple_of(j * angles, angles), angles), pl.ds(first, width)]
    last = pltpu.make_async_copy(fin.at[pl.ds(spot * each, each)], view, lsem.at[1])
    final = []
    for r in range(1, size):
        peer = lax.rem(spot + r, size)
        final.append(
            pltpu.make_async_remote_copy(
                src_ref=fin.at[pl.ds(peer * each, each)],
                dst_ref=view,
                send_sem=fs.at[r - 1],
                recv_sem=fr.at[r - 1],
                device_id=at(plane, peer, grp),
                device_id_type=MESH,
            )
        )
    for copy in final:
        copy.start()
    last.start()
    last.wait()
    for copy in final:
        copy.wait()


def local(offsets, slant_weights, live, block_tile, image_slot):
    shots, grp = lax.axis_size("shot"), lax.axis_size("grp")
    planes, size = shots // PAIR, PAIR * grp
    blocks = block_tile.shape[0]
    hs, depth = offsets.shape[1:]
    angles = slant_weights.shape[0]
    width = 2 * depth // size
    tile_rows = IMG_DEV * grp
    images = shots * tile_rows
    per_plane = images // planes
    any_space = pl.BlockSpec(memory_space=pl.ANY)
    vmem = pl.BlockSpec(memory_space=pltpu.VMEM)
    dma = pltpu.SemaphoreType.DMA

    cutoff = jnp.sum(live.reshape(blocks, 2, angles), axis=2)
    image = block_tile[:, 0] * tile_rows + image_slot
    index = jnp.arange(blocks, dtype=jnp.int32)
    same = (image[:, None] == image[None, :]) & (index[None, :] < index[:, None])
    before = jnp.max(jnp.where(same, index[None, :], -1), axis=1)
    found = image[None, :] == jnp.arange(images, dtype=jnp.int32)[:, None]
    final = jnp.max(jnp.where(found, index[None, :], -1), axis=1)
    final = jnp.where(final < 0, blocks, final).reshape(images // LANES, LANES)
    before = jnp.where(before < 0, blocks, before)
    aux = jnp.concatenate([before[None], cutoff.T], axis=0)
    aux = jnp.concatenate([jnp.pad(aux, ((0, 0), (0, LANES - blocks))), final], axis=0)
    aux = jnp.pad(aux, ((0, -aux.shape[0] % 8), (0, 0)))

    part, mom = pl.pallas_call(
        functools.partial(exchange_kernel, grp),
        out_shape=(
            jax.ShapeDtypeStruct((images, angles, width), jnp.bfloat16),
            jax.ShapeDtypeStruct((angles, LANES), jnp.float32),
        ),
        in_specs=[any_space, vmem, vmem],
        out_specs=(vmem, vmem),
        scratch_shapes=[
            pltpu.VMEM((size, blocks, hs, width), jnp.bfloat16),
            pltpu.VMEM((size,) + aux.shape, jnp.int32),
            pltpu.SMEM((size,) + aux.shape, jnp.int32),
            pltpu.VMEM((images, angles, width), jnp.float32),
            pltpu.VMEM((blocks + 1, angles, width), jnp.float32),
            dma((size - 1,)),
            dma((size - 1,)),
            dma((size - 1,)),
            dma((size - 1,)),
            dma((size + 1,)),
        ],
        compiler_params=pltpu.CompilerParams(
            collective_id=0, has_side_effects=True, vmem_limit_bytes=62 * 1024 * 1024
        ),
        name="exchange",
    )(offsets.reshape(blocks, 2, hs, depth), aux, slant_weights)

    moments = (angles, LANES)
    return pl.pallas_call(
        functools.partial(gather_kernel, grp),
        out_shape=jax.ShapeDtypeStruct((IMG_DEV, 2 * angles, depth), jnp.bfloat16),
        in_specs=[any_space, vmem],
        out_specs=any_space,
        scratch_shapes=[
            pltpu.VMEM((planes - 1, per_plane, angles, width), jnp.bfloat16),
            pltpu.VMEM((per_plane, angles, width), jnp.bfloat16),
            pltpu.VMEM((per_plane, angles, width), jnp.bfloat16),
            pltpu.VMEM((size - 1,) + moments, jnp.float32),
            pltpu.VMEM((planes - 1,) + moments, jnp.float32),
            pltpu.VMEM(moments, jnp.float32),
            dma((planes - 1,)),
            dma((planes - 1,)),
            dma((size - 1,)),
            dma((size - 1,)),
            dma((planes - 1,)),
            dma((planes - 1,)),
            dma((size - 1,)),
            dma((size - 1,)),
            dma((2,)),
        ],
        compiler_params=pltpu.CompilerParams(
            collective_id=1, has_side_effects=True, vmem_limit_bytes=60 * 1024 * 1024
        ),
        name="gather",
    )(part, mom)


def solution(mesh):
    placed = (
        P(("shot", "grp"), None, None),
        P(),
        P(("shot", "grp"), None),
        P(("shot", "grp"), None),
        P(("shot", "grp")),
    )
    return jax.shard_map(
        local, mesh=mesh, in_specs=placed, out_specs=P(("shot", "grp"), None, None), check_vma=False
    )
```

```python
import functools

import jax
import jax.numpy as jnp
from jax import lax
from jax.experimental import pallas as pl
from jax.experimental.pallas import tpu as pltpu
from jax.sharding import PartitionSpec as P

IMG_DEV = 4
PAIR = 2
LANES = 128
UNROLL = 8
MESH = pl.DeviceIdType.MESH


def place(grp):
    shot, g = lax.axis_index("shot"), lax.axis_index("grp")
    return lax.div(shot, PAIR), lax.rem(shot, PAIR) * grp + g


def at(plane, spot, grp):
    return (plane * PAIR + lax.div(spot, grp), lax.rem(spot, grp))


def share(spot, width, depth):
    start = spot * width
    return lax.div(start, depth), pl.multiple_of(lax.rem(start, depth), LANES)


def relative(spot, grp, r):
    mid = grp // 2
    pair, rest = lax.div(spot, grp), lax.rem(spot, grp)
    m, c = lax.div(rest, 2), lax.rem(rest, 2)
    rp, rm, rc = r // grp, (r % grp) // 2, r % 2
    pair, m, c = lax.rem(pair + rp, PAIR), lax.rem(m + rm, mid), lax.rem(c + rc, 2)
    return (pair * mid + m) * 2 + c


def orders(grp):
    size = PAIR * grp
    far = list(range(grp + 2, size))
    side = list(range(grp, grp + 2))
    ahead = list(range(2, grp))
    turn = []
    for i in range(max(len(far), len(ahead))):
        for group in (far, side, ahead):
            turn += group[i : i + 1]
    return [1] + turn


def exchange_kernel(
    grp, off, aux, w, part, mom, raw, aux_in, codes, acc, seg, send, recv, asend, arecv, lsem
):
    size = PAIR * grp
    plane, spot = place(grp)
    blocks, depth, width = off.shape[0], off.shape[3], raw.shape[3]
    angles, images = w.shape[0], acc.shape[0]
    j, first = share(spot, width, depth)
    mine = pltpu.make_async_copy(off.at[:, j, :, pl.ds(first, width)], raw.at[0], lsem.at[0])
    mine.start()
    own_codes = pltpu.make_async_copy(aux, codes.at[0], lsem.at[1])
    own_codes.start()
    barrier = pltpu.get_barrier_semaphore()
    for r in range(1, size):
        pl.semaphore_signal(
            barrier, inc=1, device_id=at(plane, relative(spot, grp, r), grp), device_id_type=MESH
        )
    pl.semaphore_wait(barrier, size - 1)
    data, notes = {}, {}
    for r in orders(grp):
        peer = relative(spot, grp, r)
        pj, pfirst = share(peer, width, depth)
        dev = at(plane, peer, grp)
        notes[r] = pltpu.make_async_remote_copy(
            src_ref=aux,
            dst_ref=aux_in.at[r],
            send_sem=asend.at[r - 1],
            recv_sem=arecv.at[r - 1],
            device_id=dev,
            device_id_type=MESH,
        )
        data[r] = pltpu.make_async_remote_copy(
            src_ref=off.at[:, pj, :, pl.ds(pfirst, width)],
            dst_ref=raw.at[r],
            send_sem=send.at[r - 1],
            recv_sem=recv.at[r - 1],
            device_id=dev,
            device_id_type=MESH,
        )
    for r in orders(grp):
        notes[r].start()
    for r in orders(grp):
        data[r].start()

    acc[...] = jnp.zeros_like(acc)
    seg[blocks] = jnp.zeros((angles, width), jnp.float32)
    row = lax.broadcasted_iota(jnp.int32, (angles, width), 0)
    weights = w[...]
    square = jnp.zeros((angles, width), jnp.float32)
    count = jnp.zeros((angles, width), jnp.float32)
    for r in [0] + orders(grp):
        if r:
            notes[r].wait()
            code = pltpu.make_async_copy(aux_in.at[r], codes.at[r], lsem.at[r + 1])
            code.start()
            code.wait()
            data[r].wait()
        else:
            own_codes.wait()
            mine.wait()

        def slant(i, carry, r=r):
            square, count = carry
            start = i * UNROLL
            x = jnp.concatenate([raw[r, start + t] for t in range(UNROLL)], axis=1)
            y = jnp.dot(weights, x, preferred_element_type=jnp.float32)
            for t in range(UNROLL):
                alive = row < codes[r, 1 + j, start + t]
                slanted = jnp.where(alive, y[:, t * width : (t + 1) * width], 0.0)
                slanted = slanted.astype(jnp.bfloat16).astype(jnp.float32)
                square += slanted * slanted
                count += jnp.where(alive, 1.0, 0.0)
                seg[start + t] = slanted + seg[codes[r, 0, start + t]]
            return square, count

        square, count = lax.fori_loop(0, blocks // UNROLL, slant, (square, count))

        def stack(i, _, r=r):
            start = i * UNROLL
            line, column = lax.div(start, LANES), lax.rem(start, LANES)
            for t in range(UNROLL):
                acc[start + t] += seg[codes[r, 3 + line, column + t]]
            return 0

        lax.fori_loop(0, images // UNROLL, stack, 0)

    def narrow(i, _):
        start = pl.multiple_of(i * UNROLL, UNROLL)
        part[pl.ds(start, UNROLL)] = acc[pl.ds(start, UNROLL)].astype(jnp.bfloat16)
        return 0

    lax.fori_loop(0, images // UNROLL, narrow, 0)
    lane = lax.broadcasted_iota(jnp.int32, (angles, LANES), 1)
    square = jnp.sum(square, axis=1, keepdims=True)
    count = jnp.sum(count, axis=1, keepdims=True)
    both = jnp.where(lane == 0, square, jnp.where(lane == 1, count, 0.0))
    both = jnp.concatenate([both, jnp.zeros((LANES - angles, LANES), jnp.float32)], axis=0)
    mom[...] = both.T[: mom.shape[0]]


def gather_kernel(
    grp, part, mom, out, held, total, fin, pin, qin, half_sum, zs, zr, ps, pr, qs, qr, fs, fr, lsem
):
    size = PAIR * grp
    planes = held.shape[1] + 1
    plane, spot = place(grp)
    pieces, rows, angles, width = held.shape[2:]
    depth = out.shape[2]
    chunk = pieces * rows
    lower = jnp.where(plane < planes // 2, 1, 0)
    barrier = pltpu.get_barrier_semaphore()
    for r in range(1, size):
        pl.semaphore_signal(
            barrier, inc=1, device_id=at(plane, lax.rem(spot + r, size), grp), device_id_type=MESH
        )
    for r in range(1, planes):
        pl.semaphore_signal(
            barrier, inc=1, device_id=at(lax.rem(plane + r, planes), spot, grp), device_id_type=MESH
        )
    pl.semaphore_wait(barrier, size + planes - 2)

    def along(up):
        spot_on_line = plane * up + (planes - 1 - plane) * (1 - up)
        following = lax.rem(plane + 2 * up - 1 + planes, planes)
        return 1 - up, spot_on_line, following

    def rows_of(up, s, h):
        target = (planes - 1 - s) * up + s * (1 - up)
        return target * chunk + h * rows

    def hop(up, s, h, source):
        way, _, following = along(up)
        return pltpu.make_async_remote_copy(
            src_ref=source,
            dst_ref=held.at[way, s, h],
            send_sem=zs.at[way, s, h],
            recv_sem=zr.at[way, s, h],
            device_id=at(following, spot, grp),
            device_id_type=MESH,
        )

    def begin(s):
        @pl.when(along(lower)[1] == 0)
        def _():
            for h in range(pieces):
                hop(lower, s, h, part.at[pl.ds(rows_of(lower, s, h), rows)]).start()

    def step(up, s, h):
        way, here, _ = along(up)
        end = planes - 1 - s

        @pl.when((here > 0) & (here <= end))
        def _():
            hop(up, s, h, held.at[way, s, h]).wait_recv()

        @pl.when((here > 0) & (here < end))
        def _():
            start = rows_of(up, s, h)

            def add(i, _):
                value = held[way, s, h, i].astype(jnp.float32) + part[start + i].astype(jnp.float32)
                held[way, s, h, i] = value.astype(jnp.bfloat16)
                return 0

            lax.fori_loop(0, rows, add, 0)
            hop(up, s, h, held.at[way, s, h]).start()

        @pl.when((here > 0) & (here == end))
        def _():
            def add(i, _):
                total[h * rows + i] += held[way, s, h, i].astype(jnp.float32)
                return 0

            lax.fori_loop(0, rows, add, 0)

    def finish(up, s, h):
        way, here, _ = along(up)

        @pl.when(here < planes - 1 - s)
        def _():
            hop(up, s, h, held.at[way, s, h]).wait_send()

    near = [
        pltpu.make_async_remote_copy(
            src_ref=mom,
            dst_ref=pin.at[r - 1],
            send_sem=ps.at[r - 1],
            recv_sem=pr.at[r - 1],
            device_id=at(plane, lax.rem(spot + r, size), grp),
            device_id_type=MESH,
        )
        for r in range(1, size)
    ]
    for copy in near:
        copy.start()
    begin(0)
    total[...] = part[pl.ds(plane * chunk, chunk)].astype(jnp.float32)
    moments = mom[...]
    for copy in near:
        copy.wait()
    for r in range(1, size):
        moments += pin[r - 1]
    half_sum[...] = moments
    wide = [
        pltpu.make_async_remote_copy(
            src_ref=half_sum,
            dst_ref=qin.at[r - 1],
            send_sem=qs.at[r - 1],
            recv_sem=qr.at[r - 1],
            device_id=at(lax.rem(plane + r, planes), spot, grp),
            device_id_type=MESH,
        )
        for r in range(1, planes)
    ]
    for copy in wide:
        copy.start()
    for s in range(1, planes - 1):
        begin(s)
    for s in range(planes - 1):
        for up in (lower, 1 - lower):
            for h in range(pieces):
                step(up, s, h)
    for copy in wide:
        copy.wait()
    moments = half_sum[...]
    for r in range(1, planes):
        moments += qin[r - 1]
    gain = lax.rsqrt(moments[0:1] / moments[1:2] + 1e-06)
    gain = jnp.broadcast_to(gain, (LANES, LANES)).T[:angles]

    def body(i, _):
        fin[i] = (total[i] * gain).astype(jnp.bfloat16)
        return 0

    lax.fori_loop(0, chunk, body, 0)

    each = chunk // size
    j, first = share(spot, width, depth)
    view = out.at[:, pl.ds(pl.multiple_of(j * angles, angles), angles), pl.ds(first, width)]
    last = pltpu.make_async_copy(fin.at[pl.ds(spot * each, each)], view, lsem.at[1])
    final = []
    for r in range(1, size):
        peer = lax.rem(spot + r, size)
        final.append(
            pltpu.make_async_remote_copy(
                src_ref=fin.at[pl.ds(peer * each, each)],
                dst_ref=view,
                send_sem=fs.at[r - 1],
                recv_sem=fr.at[r - 1],
                device_id=at(plane, peer, grp),
                device_id_type=MESH,
            )
        )
    for copy in final:
        copy.start()
    last.start()
    last.wait()
    for copy in final:
        copy.wait()
    for s in range(planes - 1):
        for up in (lower, 1 - lower):
            for h in range(pieces):
                finish(up, s, h)


def local(offsets, slant_weights, live, block_tile, image_slot):
    shots, grp = lax.axis_size("shot"), lax.axis_size("grp")
    planes, size = shots // PAIR, PAIR * grp
    blocks = block_tile.shape[0]
    hs, depth = offsets.shape[1:]
    angles = slant_weights.shape[0]
    width = 2 * depth // size
    tile_rows = IMG_DEV * grp
    images = shots * tile_rows
    per_plane = images // planes
    any_space = pl.BlockSpec(memory_space=pl.ANY)
    vmem = pl.BlockSpec(memory_space=pltpu.VMEM)
    dma = pltpu.SemaphoreType.DMA

    cutoff = jnp.sum(live.reshape(blocks, 2, angles), axis=2)
    image = block_tile[:, 0] * tile_rows + image_slot
    index = jnp.arange(blocks, dtype=jnp.int32)
    same = (image[:, None] == image[None, :]) & (index[None, :] < index[:, None])
    before = jnp.max(jnp.where(same, index[None, :], -1), axis=1)
    found = image[None, :] == jnp.arange(images, dtype=jnp.int32)[:, None]
    final = jnp.max(jnp.where(found, index[None, :], -1), axis=1)
    final = jnp.where(final < 0, blocks, final).reshape(images // LANES, LANES)
    before = jnp.where(before < 0, blocks, before)
    aux = jnp.concatenate([before[None], cutoff.T], axis=0)
    aux = jnp.concatenate([jnp.pad(aux, ((0, 0), (0, LANES - blocks))), final], axis=0)
    aux = jnp.pad(aux, ((0, -aux.shape[0] % 8), (0, 0)))

    part, mom = pl.pallas_call(
        functools.partial(exchange_kernel, grp),
        out_shape=(
            jax.ShapeDtypeStruct((images, angles, width), jnp.bfloat16),
            jax.ShapeDtypeStruct((8, LANES), jnp.float32),
        ),
        in_specs=[any_space, vmem, vmem],
        out_specs=(vmem, vmem),
        scratch_shapes=[
            pltpu.VMEM((size, blocks, hs, width), jnp.bfloat16),
            pltpu.VMEM((size,) + aux.shape, jnp.int32),
            pltpu.SMEM((size,) + aux.shape, jnp.int32),
            pltpu.VMEM((images, angles, width), jnp.float32),
            pltpu.VMEM((blocks + 1, angles, width), jnp.float32),
            dma((size - 1,)),
            dma((size - 1,)),
            dma((size - 1,)),
            dma((size - 1,)),
            dma((size + 1,)),
        ],
        compiler_params=pltpu.CompilerParams(
            collective_id=0, has_side_effects=True, vmem_limit_bytes=62 * 1024 * 1024
        ),
        name="exchange",
    )(offsets.reshape(blocks, 2, hs, depth), aux, slant_weights)

    moments = (8, LANES)
    pieces = 2
    lines = (2, planes - 1, pieces)
    return pl.pallas_call(
        functools.partial(gather_kernel, grp),
        out_shape=jax.ShapeDtypeStruct((IMG_DEV, 2 * angles, depth), jnp.bfloat16),
        in_specs=[vmem, vmem],
        out_specs=any_space,
        scratch_shapes=[
            pltpu.VMEM(lines + (per_plane // pieces, angles, width), jnp.bfloat16),
            pltpu.VMEM((per_plane, angles, width), jnp.float32),
            pltpu.VMEM((per_plane, angles, width), jnp.bfloat16),
            pltpu.VMEM((size - 1,) + moments, jnp.float32),
            pltpu.VMEM((planes - 1,) + moments, jnp.float32),
            pltpu.VMEM(moments, jnp.float32),
            dma(lines),
            dma(lines),
            dma((size - 1,)),
            dma((size - 1,)),
            dma((planes - 1,)),
            dma((planes - 1,)),
            dma((size - 1,)),
            dma((size - 1,)),
            dma((2,)),
        ],
        compiler_params=pltpu.CompilerParams(
            collective_id=1, has_side_effects=True, vmem_limit_bytes=60 * 1024 * 1024
        ),
        name="gather",
    )(part, mom)


def solution(mesh):
    placed = (
        P(("shot", "grp"), None, None),
        P(),
        P(("shot", "grp"), None),
        P(("shot", "grp"), None),
        P(("shot", "grp")),
    )
    return jax.shard_map(
        local, mesh=mesh, in_specs=placed, out_specs=P(("shot", "grp"), None, None), check_vma=False
    )
```

```python
import functools

import jax
import jax.numpy as jnp
from jax import lax
from jax.experimental import pallas as pl
from jax.experimental.pallas import tpu as pltpu
from jax.sharding import PartitionSpec as P

IMG_DEV = 4
PAIR = 2
LANES = 128
UNROLL = 8
MESH = pl.DeviceIdType.MESH


def place(grp):
    shot, g = lax.axis_index("shot"), lax.axis_index("grp")
    return lax.div(shot, PAIR), lax.rem(shot, PAIR) * grp + g


def at(plane, spot, grp):
    return (plane * PAIR + lax.div(spot, grp), lax.rem(spot, grp))


def share(spot, width, depth):
    start = spot * width
    return lax.div(start, depth), pl.multiple_of(lax.rem(start, depth), LANES)


def relative(spot, grp, r):
    mid = grp // 2
    pair, rest = lax.div(spot, grp), lax.rem(spot, grp)
    m, c = lax.div(rest, 2), lax.rem(rest, 2)
    rp, rm, rc = r // grp, (r % grp) // 2, r % 2
    pair, m, c = lax.rem(pair + rp, PAIR), lax.rem(m + rm, mid), lax.rem(c + rc, 2)
    return (pair * mid + m) * 2 + c


def orders(grp):
    size = PAIR * grp
    far = list(range(grp + 2, size))
    side = list(range(grp, grp + 2))
    ahead = list(range(2, grp))
    turn = []
    for i in range(max(len(far), len(ahead))):
        for group in (far, side, ahead):
            turn += group[i : i + 1]
    return [1] + turn


def exchange_kernel(
    grp, off, aux, w_in, part, mom, w, raw, aux_in, codes, acc, seg, send, recv, asend, arecv, lsem
):
    size = PAIR * grp
    plane, spot = place(grp)
    blocks, depth, width = off.shape[0], off.shape[3], raw.shape[3]
    angles, images = w.shape[1], acc.shape[0]
    j, first = share(spot, width, depth)
    mine = pltpu.make_async_copy(off.at[:, j, :, pl.ds(first, width)], raw.at[0], lsem.at[0])
    mine.start()
    own_codes = pltpu.make_async_copy(aux, codes.at[0], lsem.at[1])
    own_codes.start()
    weigh = pltpu.make_async_copy(w_in, w, lsem.at[size + 1])
    weigh.start()
    barrier = pltpu.get_barrier_semaphore()
    for r in range(1, size):
        pl.semaphore_signal(
            barrier, inc=1, device_id=at(plane, relative(spot, grp, r), grp), device_id_type=MESH
        )
    pl.semaphore_wait(barrier, size - 1)
    data, notes = {}, {}
    for r in orders(grp):
        peer = relative(spot, grp, r)
        pj, pfirst = share(peer, width, depth)
        dev = at(plane, peer, grp)
        notes[r] = pltpu.make_async_remote_copy(
            src_ref=aux,
            dst_ref=aux_in.at[r],
            send_sem=asend.at[r - 1],
            recv_sem=arecv.at[r - 1],
            device_id=dev,
            device_id_type=MESH,
        )
        data[r] = pltpu.make_async_remote_copy(
            src_ref=off.at[:, pj, :, pl.ds(pfirst, width)],
            dst_ref=raw.at[r],
            send_sem=send.at[r - 1],
            recv_sem=recv.at[r - 1],
            device_id=dev,
            device_id_type=MESH,
        )
    for r in orders(grp):
        notes[r].start()
    for r in orders(grp):
        data[r].start()

    acc[...] = jnp.zeros_like(acc)
    seg[blocks] = jnp.zeros((angles, width), jnp.float32)
    row = lax.broadcasted_iota(jnp.int32, (angles, width), 0)
    weigh.wait()
    weights = w[...].astype(jnp.float32).T.astype(jnp.bfloat16)
    square = jnp.zeros((angles, width), jnp.float32)
    count = jnp.zeros((angles, width), jnp.float32)
    for r in [0] + orders(grp):
        if r:
            notes[r].wait()
            code = pltpu.make_async_copy(aux_in.at[r], codes.at[r], lsem.at[r + 1])
            code.start()
            code.wait()
            data[r].wait()
        else:
            own_codes.wait()
            mine.wait()

        def slant(i, carry, r=r):
            square, count = carry
            start = i * UNROLL
            x = jnp.concatenate([raw[r, start + t] for t in range(UNROLL)], axis=1)
            y = jnp.dot(weights, x, preferred_element_type=jnp.float32)
            for t in range(UNROLL):
                alive = row < codes[r, 1 + j, start + t]
                slanted = jnp.where(alive, y[:, t * width : (t + 1) * width], 0.0)
                slanted = slanted.astype(jnp.bfloat16).astype(jnp.float32)
                square += slanted * slanted
                count += jnp.where(alive, 1.0, 0.0)
                seg[start + t] = slanted + seg[codes[r, 0, start + t]]
            return square, count

        square, count = lax.fori_loop(0, blocks // UNROLL, slant, (square, count))

        def stack(i, _, r=r):
            start = i * UNROLL
            line, column = lax.div(start, LANES), lax.rem(start, LANES)
            for t in range(UNROLL):
                acc[start + t] += seg[codes[r, 3 + line, column + t]]
            return 0

        lax.fori_loop(0, images // UNROLL, stack, 0)

    def narrow(i, _):
        start = pl.multiple_of(i * UNROLL, UNROLL)
        part[pl.ds(start, UNROLL)] = acc[pl.ds(start, UNROLL)].astype(jnp.bfloat16)
        return 0

    lax.fori_loop(0, images // UNROLL, narrow, 0)
    lane = lax.broadcasted_iota(jnp.int32, (angles, LANES), 1)
    square = jnp.sum(square, axis=1, keepdims=True)
    count = jnp.sum(count, axis=1, keepdims=True)
    both = jnp.where(lane == 0, square, jnp.where(lane == 1, count, 0.0))
    both = jnp.concatenate([both, jnp.zeros((LANES - angles, LANES), jnp.float32)], axis=0)
    mom[...] = both.T[: mom.shape[0]]


def gather_kernel(
    grp, part, mom, out, held, total, fin, pin, qin, half_sum, zs, zr, ps, pr, qs, qr, fs, fr, lsem
):
    size = PAIR * grp
    planes = held.shape[1] + 1
    plane, spot = place(grp)
    pieces, rows, angles, width = held.shape[2:]
    depth = out.shape[2]
    chunk = pieces * rows
    lower = jnp.where(plane < planes // 2, 1, 0)
    barrier = pltpu.get_barrier_semaphore()
    for r in range(1, size):
        pl.semaphore_signal(
            barrier, inc=1, device_id=at(plane, lax.rem(spot + r, size), grp), device_id_type=MESH
        )
    for r in range(1, planes):
        pl.semaphore_signal(
            barrier, inc=1, device_id=at(lax.rem(plane + r, planes), spot, grp), device_id_type=MESH
        )
    pl.semaphore_wait(barrier, size + planes - 2)

    def along(up):
        spot_on_line = plane * up + (planes - 1 - plane) * (1 - up)
        following = lax.rem(plane + 2 * up - 1 + planes, planes)
        return 1 - up, spot_on_line, following

    def rows_of(up, s, h):
        target = (planes - 1 - s) * up + s * (1 - up)
        return target * chunk + h * rows

    def hop(up, s, h, source):
        way, _, following = along(up)
        return pltpu.make_async_remote_copy(
            src_ref=source,
            dst_ref=held.at[way, s, h],
            send_sem=zs.at[way, s, h],
            recv_sem=zr.at[way, s, h],
            device_id=at(following, spot, grp),
            device_id_type=MESH,
        )

    def begin(s):
        @pl.when(along(lower)[1] == 0)
        def _():
            for h in range(pieces):
                hop(lower, s, h, part.at[pl.ds(rows_of(lower, s, h), rows)]).start()

    def step(up, s, h):
        way, here, _ = along(up)
        end = planes - 1 - s

        @pl.when((here > 0) & (here <= end))
        def _():
            hop(up, s, h, held.at[way, s, h]).wait_recv()

        @pl.when((here > 0) & (here < end))
        def _():
            start = rows_of(up, s, h)

            def add(i, _):
                value = held[way, s, h, i].astype(jnp.float32) + part[start + i].astype(jnp.float32)
                held[way, s, h, i] = value.astype(jnp.bfloat16)
                return 0

            lax.fori_loop(0, rows, add, 0)
            hop(up, s, h, held.at[way, s, h]).start()

        @pl.when((here > 0) & (here == end))
        def _():
            def add(i, _):
                total[h * rows + i] += held[way, s, h, i].astype(jnp.float32)
                return 0

            lax.fori_loop(0, rows, add, 0)

    def finish(up, s, h):
        way, here, _ = along(up)

        @pl.when(here < planes - 1 - s)
        def _():
            hop(up, s, h, held.at[way, s, h]).wait_send()

    near = [
        pltpu.make_async_remote_copy(
            src_ref=mom,
            dst_ref=pin.at[r - 1],
            send_sem=ps.at[r - 1],
            recv_sem=pr.at[r - 1],
            device_id=at(plane, lax.rem(spot + r, size), grp),
            device_id_type=MESH,
        )
        for r in range(1, size)
    ]
    for copy in near:
        copy.start()
    begin(0)
    total[...] = part[pl.ds(plane * chunk, chunk)].astype(jnp.float32)
    moments = mom[...]
    for copy in near:
        copy.wait()
    for r in range(1, size):
        moments += pin[r - 1]
    half_sum[...] = moments
    wide = [
        pltpu.make_async_remote_copy(
            src_ref=half_sum,
            dst_ref=qin.at[r - 1],
            send_sem=qs.at[r - 1],
            recv_sem=qr.at[r - 1],
            device_id=at(lax.rem(plane + r, planes), spot, grp),
            device_id_type=MESH,
        )
        for r in range(1, planes)
    ]
    for copy in wide:
        copy.start()
    for s in range(1, planes - 1):
        begin(s)
    for s in range(planes - 1):
        for up in (lower, 1 - lower):
            for h in range(pieces):
                step(up, s, h)
    for copy in wide:
        copy.wait()
    moments = half_sum[...]
    for r in range(1, planes):
        moments += qin[r - 1]
    gain = lax.rsqrt(moments[0:1] / moments[1:2] + 1e-06)
    gain = jnp.broadcast_to(gain, (LANES, LANES)).T[:angles]

    def body(i, _):
        fin[i] = (total[i] * gain).astype(jnp.bfloat16)
        return 0

    lax.fori_loop(0, chunk, body, 0)

    each = chunk // size
    j, first = share(spot, width, depth)
    view = out.at[:, pl.ds(pl.multiple_of(j * angles, angles), angles), pl.ds(first, width)]
    last = pltpu.make_async_copy(fin.at[pl.ds(spot * each, each)], view, lsem.at[1])
    final = []
    for r in range(1, size):
        peer = lax.rem(spot + r, size)
        final.append(
            pltpu.make_async_remote_copy(
                src_ref=fin.at[pl.ds(peer * each, each)],
                dst_ref=view,
                send_sem=fs.at[r - 1],
                recv_sem=fr.at[r - 1],
                device_id=at(plane, peer, grp),
                device_id_type=MESH,
            )
        )
    for copy in final:
        copy.start()
    last.start()
    last.wait()
    for copy in final:
        copy.wait()
    for s in range(planes - 1):
        for up in (lower, 1 - lower):
            for h in range(pieces):
                finish(up, s, h)


def local(offsets, slant_weights, live, block_tile, image_slot):
    shots, grp = lax.axis_size("shot"), lax.axis_size("grp")
    planes, size = shots // PAIR, PAIR * grp
    blocks = block_tile.shape[0]
    hs, depth = offsets.shape[1:]
    angles = slant_weights.shape[0]
    width = 2 * depth // size
    tile_rows = IMG_DEV * grp
    images = shots * tile_rows
    per_plane = images // planes
    any_space = pl.BlockSpec(memory_space=pl.ANY)
    vmem = pl.BlockSpec(memory_space=pltpu.VMEM)
    dma = pltpu.SemaphoreType.DMA

    cutoff = jnp.sum(live.reshape(blocks, 2, angles), axis=2)
    image = block_tile[:, 0] * tile_rows + image_slot
    index = jnp.arange(blocks, dtype=jnp.int32)
    same = (image[:, None] == image[None, :]) & (index[None, :] < index[:, None])
    before = jnp.max(jnp.where(same, index[None, :], -1), axis=1)
    found = image[None, :] == jnp.arange(images, dtype=jnp.int32)[:, None]
    final = jnp.max(jnp.where(found, index[None, :], -1), axis=1)
    final = jnp.where(final < 0, blocks, final).reshape(images // LANES, LANES)
    before = jnp.where(before < 0, blocks, before)
    aux = jnp.concatenate([before[None], cutoff.T], axis=0)
    aux = jnp.concatenate([jnp.pad(aux, ((0, 0), (0, LANES - blocks))), final], axis=0)
    aux = jnp.pad(aux, ((0, -aux.shape[0] % 8), (0, 0)))

    part, mom = pl.pallas_call(
        functools.partial(exchange_kernel, grp),
        out_shape=(
            jax.ShapeDtypeStruct((images, angles, width), jnp.bfloat16),
            jax.ShapeDtypeStruct((8, LANES), jnp.float32),
        ),
        in_specs=[any_space, vmem, any_space],
        out_specs=(vmem, vmem),
        scratch_shapes=[
            pltpu.VMEM((hs, angles), jnp.bfloat16),
            pltpu.VMEM((size, blocks, hs, width), jnp.bfloat16),
            pltpu.VMEM((size,) + aux.shape, jnp.int32),
            pltpu.SMEM((size,) + aux.shape, jnp.int32),
            pltpu.VMEM((images, angles, width), jnp.float32),
            pltpu.VMEM((blocks + 1, angles, width), jnp.float32),
            dma((size - 1,)),
            dma((size - 1,)),
            dma((size - 1,)),
            dma((size - 1,)),
            dma((size + 2,)),
        ],
        compiler_params=pltpu.CompilerParams(
            collective_id=0, has_side_effects=True, vmem_limit_bytes=62 * 1024 * 1024
        ),
        name="exchange",
    )(offsets.reshape(blocks, 2, hs, depth), aux, slant_weights.T)

    moments = (8, LANES)
    pieces = 4
    lines = (2, planes - 1, pieces)
    return pl.pallas_call(
        functools.partial(gather_kernel, grp),
        out_shape=jax.ShapeDtypeStruct((IMG_DEV, 2 * angles, depth), jnp.bfloat16),
        in_specs=[vmem, vmem],
        out_specs=any_space,
        scratch_shapes=[
            pltpu.VMEM(lines + (per_plane // pieces, angles, width), jnp.bfloat16),
            pltpu.VMEM((per_plane, angles, width), jnp.float32),
            pltpu.VMEM((per_plane, angles, width), jnp.bfloat16),
            pltpu.VMEM((size - 1,) + moments, jnp.float32),
            pltpu.VMEM((planes - 1,) + moments, jnp.float32),
            pltpu.VMEM(moments, jnp.float32),
            dma(lines),
            dma(lines),
            dma((size - 1,)),
            dma((size - 1,)),
            dma((planes - 1,)),
            dma((planes - 1,)),
            dma((size - 1,)),
            dma((size - 1,)),
            dma((2,)),
        ],
        compiler_params=pltpu.CompilerParams(
            collective_id=1, has_side_effects=True, vmem_limit_bytes=60 * 1024 * 1024
        ),
        name="gather",
    )(part, mom)


def solution(mesh):
    placed = (
        P(("shot", "grp"), None, None),
        P(),
        P(("shot", "grp"), None),
        P(("shot", "grp"), None),
        P(("shot", "grp")),
    )
    return jax.shard_map(
        local, mesh=mesh, in_specs=placed, out_specs=P(("shot", "grp"), None, None), check_vma=False
    )
```
